128 devices in a mesh: layer: 2 (over core), expert: 16 (over y, x), matrix: 4 (over z).
Axes of the slice: x: 4, y: 4, z: 4, core: 2. Of those that a mesh axis runs over, the one named last changes fastest.
Arguments:
- grads: float32 [32, 1, 2048, 768], P(('layer', 'expert'), None, 'matrix'), parts along dimension 0, may hold values from -6 to 6
- basis_out: float32 [32, 2048, 2048], P('layer', None, ('expert', 'matrix')), parts along dimension 0, may hold values from -0.125 to 0.125
- basis_in: float32 [32, 768, 768], P('layer', ('expert', 'matrix')), parts along dimension 0, may hold values from -0.21875 to 0.21875
- eigvals: float32 [32, 2048, 768], P('layer', ('expert', 'matrix')), parts along dimension 0, may hold values from 0.001 to 1
- counts: int32 [32], P(('layer', 'expert')), parts along dimension 0, may hold values from 0 to 1, as said below
- slot_query: int32 [32, 1], P(('layer', 'expert')), parts along dimension 0, may hold values from 0 to 31
Outputs:
- precond: float32 [32, 1, 2048, 768], P(('layer', 'expert'), None, 'matrix'), parts along dimension 0
- scores: float32 [64], P('layer'), parts along dimension 0
The draws below stay inside these ranges and needn't reach their ends.
There are 2 independent parts, one for each index of `layer`. The reference program is written for one: setup_inputs(seed, part) draws one part's arguments, and reference() takes and returns one part's arrays. A program takes and returns all parts, laid end to end along the dimension named above; each array names one. Nothing has to cross between parts.
Inputs may be any that keep to these rules, and one draw needn't show every extreme that they name: `counts`: some expert has no live slot and some expert has all 1.
All inputs are finite; a program needn't handle non-finite values.
Results may differ from the reference program's by a relative error of at most 0.0003.
Values sent between devices are 32-bit elements; how exact they have to be, the bound alone decides.
A program may use at most 64 MiB of HBM per device.

```python
import math
import jax
import jax.numpy as jnp
from jax import lax

D = 2048
F = 768
CAP = 1
QUERIES = 32
EXPERTS = 16


def draw_counts(key, part):
    base = jax.random.randint(key, (EXPERTS,), 0, CAP + 1)
    chosen = jax.random.randint(jax.random.fold_in(key, 7), (), 0, EXPERTS)
    offset = jax.random.randint(jax.random.fold_in(key, 11), (), 1, EXPERTS)
    emptied = (chosen + offset) % EXPERTS
    where = jnp.arange(EXPERTS)
    filled = jnp.where(where == chosen, CAP, base)
    return jnp.where(where == emptied, 0, filled).astype(jnp.int32)


def plant(values, stream_key, least, top_value):
    shape = values.shape
    place = [jax.random.randint(jax.random.fold_in(stream_key, axis), (), 0, shape[axis]) for axis in range(len(shape))]
    values = values.at[tuple(place)].set(least)
    longest = shape.index(max(shape))
    place[longest] = (place[longest] + 1) % shape[longest]
    return values.at[tuple(place)].set(top_value)


def level_of(stream_key, dims, shards, low, largest):
    def one(axis_at, parts):
        steps = jax.random.uniform(jax.random.fold_in(jax.random.fold_in(stream_key, 6), axis_at), (parts,), jnp.float32, low / len(shards), largest / len(shards))
        return jnp.repeat(jnp.exp(steps), dims[axis_at] // parts).reshape((-1,) + (1,) * (len(dims) - axis_at - 1))

    level = one(*shards[0])
    for cut in shards[1:]:
        level = level * one(*cut)
    return level


def scatter_about(own_key, dims, spread, most, shards=(), held_as=jnp.bfloat16):
    values = spread * jax.random.normal(own_key, dims, jnp.float32)
    if shards:
        values = values * level_of(own_key, dims, shards, -0.22, 0.18)
    return jnp.clip(values, -most, most).astype(held_as)


def setup_inputs(seed: int = 0, part: int = 0) -> dict:
    arg_keys = jax.random.split(jax.random.key(seed), 7)
    own_keys = jax.random.split(jax.random.fold_in(arg_keys[6], part), 7)
    grads = scatter_about(own_keys[0], (EXPERTS, CAP, D, F), 1.0, 6.0, ((0, 16), (2, 4)), jnp.float32)
    basis_out = scatter_about(own_keys[1], (EXPERTS, D, D), D ** -0.5, 0.125, ((2, 64),), jnp.float32)
    basis_in = scatter_about(own_keys[2], (EXPERTS, F, F), F ** -0.5, 0.21875, ((1, 64),), jnp.float32)
    eigvals = jnp.clip(jnp.exp(math.log(1.0) - 6.9077552 * jax.random.uniform(own_keys[3], (EXPERTS, D, F), jnp.float32) ** level_of(own_keys[3], (EXPERTS, D, F), ((1, 64),), -0.2, 0.2)), 0.001, 1.0)
    counts = draw_counts(jax.random.fold_in(jax.random.fold_in(arg_keys[6], part), 71), part)
    slot_query = plant(jax.random.randint(own_keys[5], (EXPERTS, CAP), 0, QUERIES), jax.random.fold_in(own_keys[5], 1), 0, QUERIES - 1).astype(jnp.int32)
    return {"grads": grads, "basis_out": basis_out, "basis_in": basis_in, "eigvals": eigvals, "counts": counts, "slot_query": slot_query}


damping_fixed = 0.05
highest = lax.Precision.HIGHEST


def one_expert(items):
    grads_e, basis_out_e, basis_in_e, eigvals_e, count_e, queries_e = items
    outputs = []
    contrib = jnp.zeros((QUERIES,), jnp.float32)
    targets = jnp.arange(QUERIES, dtype=jnp.int32)
    for slot_index in range(CAP):
        gradient = grads_e[slot_index]
        rotated = jnp.dot(jnp.dot(basis_out_e.T, gradient, precision=highest), basis_in_e, precision=highest)
        scaled = rotated / (eigvals_e + damping_fixed)
        back = jnp.dot(scaled, basis_in_e.T, precision=highest)
        result = jnp.dot(basis_out_e, back, precision=highest)
        live = (slot_index < count_e).astype(jnp.float32)
        result = result * live
        outputs.append(result)
        value = jnp.sum(gradient * result) / (D * F)
        onehot = (queries_e[slot_index] == targets).astype(jnp.float32)
        contrib = contrib + value * onehot
    return jnp.stack(outputs), contrib


def reference(grads, basis_out, basis_in, eigvals, counts, slot_query):
    precond, contribs = lax.map(one_expert, (grads, basis_out, basis_in, eigvals, counts, slot_query))
    scores = jnp.sum(contribs, axis=0)
    return precond, scores
```

```python
import functools

import jax
import jax.numpy as jnp
from jax import lax
from jax.experimental import pallas as pl
from jax.experimental.pallas import tpu as pltpu
from jax.sharding import PartitionSpec as P

MESH = pl.DeviceIdType.MESH
QUERIES = 32
SIDE = 4
PLANES = 4
EXPERTS = 16
DAMPING = 0.05
BF16 = jnp.bfloat16
F32 = jnp.float32

ORDER = [(0, 0)] + sorted(
    [(dy, dx) for dy in range(SIDE) for dx in range(SIDE) if dy or dx],
    key=lambda d: min(d[0], SIDE - d[0]) + min(d[1], SIDE - d[1]),
)
CHUNKS = 4
PER_CHUNK = EXPERTS // CHUNKS


def split(x):
    high = x.astype(BF16)
    return high, (x - high.astype(F32)).astype(BF16)


def dot(a, b):
    return lax.dot_general(a, b, (((1,), (0,)), ((), ())), preferred_element_type=F32)


def dot_t(a, b):
    return lax.dot_general(a, b, (((1,), (1,)), ((), ())), preferred_element_type=F32)


def wait_bytes(ref, sem):
    pltpu.make_async_copy(ref, ref, sem).wait()


def kernel(
    g, bo, bi, lam, counts, query, out, scores,
    g_all, bo_all, bi_all, lam_all, g_hi, g_lo, bo_hi, bo_lo, bi_hi, bi_lo,
    bt_hi, bt_lo, snd, own, rcv, fin, score_acc, scz, scx, scy,
    loc_sem, g_send, g_recv, bi_send, bi_recv, rel_send, rel_recv,
    bo_send, bo_recv, lam_send, lam_recv, out_send, out_recv, fin_sem,
    sc_send, sc_recv,
):
    layer = lax.axis_index("layer")
    e = lax.axis_index("expert")
    m = lax.axis_index("matrix")
    y, x = e // SIDE, lax.rem(e, SIDE)
    active = lax.rem(m + layer, 2) == 0
    rows = g.shape[0]
    piece = bo.shape[1]
    half = piece // 2
    slot_rows = 2 * piece
    chunk_rows = PER_CHUNK * slot_rows
    width = bo.shape[2]
    inner = g.shape[1]
    parts = snd.shape[1]
    tall = snd.shape[2]

    def plane(step):
        return lax.rem(m + step, PLANES)

    def place(d):
        return lax.rem(y + d[0], SIDE) * SIDE + lax.rem(x + d[1], SIDE)

    def remote(src, dst, send, recv, expert, matrix):
        return pltpu.make_async_remote_copy(
            src_ref=src,
            dst_ref=dst,
            send_sem=send,
            recv_sem=recv,
            device_id={"layer": layer, "expert": expert, "matrix": matrix},
            device_id_type=MESH,
        )

    g_steps = {1: 0, 3: 1, 2: 2}

    def send_g(step):
        return remote(g, g_all.at[m], g_send.at[g_steps[step]], g_recv.at[g_steps[step]], e, plane(step))

    bi_own = pltpu.make_async_copy(bi.at[e], bi_all.at[m, e], loc_sem.at[0])
    g_own = pltpu.make_async_copy(g, g_all.at[m], loc_sem.at[1])
    bo_own = pltpu.make_async_copy(bo.at[e], bo_all.at[pl.ds(0, piece)], loc_sem.at[2])
    lam_own = pltpu.make_async_copy(lam.at[e], lam_all.at[pl.ds(0, piece)], loc_sem.at[3])

    bi_own.start()
    for s in range(1, EXPERTS):
        to = place(ORDER[s])
        remote(bi.at[to], bi_all.at[m, e], bi_send, bi_recv, to, m).start()

    def send_slot(s, is_active):
        to = place(ORDER[s])
        chunk = s // PER_CHUNK
        base = s * slot_rows
        if is_active:
            remote(bo.at[to], bo_all.at[pl.ds(base, piece)], bo_send, bo_recv.at[chunk], to, m).start()
            remote(lam.at[to], lam_all.at[pl.ds(base, piece)], lam_send, lam_recv.at[chunk], to, m).start()
        else:
            for which, step in enumerate((1, 3)):
                mine = pl.ds(which * half, half)
                there = pl.ds(base + piece + which * half, half)
                remote(bo.at[to, mine], bo_all.at[there], bo_send, bo_recv.at[chunk], to, plane(step)).start()
                remote(lam.at[to, mine], lam_all.at[there], lam_send, lam_recv.at[chunk], to, plane(step)).start()

    def wait_bi_plane():
        bi_own.wait()
        wait_bytes(bi_all.at[0, pl.ds(0, EXPERTS - 1)], bi_recv)

    def send_relay(step):
        return remote(
            bi_all.at[m], bi_all.at[m], rel_send.at[g_steps[step]], rel_recv.at[g_steps[step]], e, plane(step)
        )

    def score_round(buf, me, index, step):
        copies = []
        for t in range(1, 4):
            if step == "z":
                where = (e, plane(t))
            elif step == "x":
                where = (place((0, t)), m)
            else:
                where = (place((t, 0)), m)
            copies.append(
                remote(buf.at[me], buf.at[me], sc_send.at[3 * index + t - 1], sc_recv.at[3 * index + t - 1], *where)
            )
        return copies

    rounds = [score_round(scz, m, 0, "z"), score_round(scx, x, 1, "x"), score_round(scy, y, 2, "y")]

    def start_all(copies):
        for c in copies:
            c.start()

    def wait_all(copies):
        for c in copies:
            c.wait()

    def total(buf):
        return (buf[0] + buf[1]) + (buf[2] + buf[3])

    def out_copy(step, part, where):
        index = {1: 0, 3: 1, 2: 2}[step]
        return remote(
            snd.at[index, part], rcv.at[where, part], out_send.at[index, part], out_recv.at[where, part], e, plane(step)
        )

    def finish(part, value):
        live = jnp.where(counts[0] > 0, 1.0, 0.0).astype(F32)
        fin[part] = jnp.transpose(value * live)
        pltpu.make_async_copy(fin.at[part], out.at[:, pl.ds(part * tall, tall)], fin_sem.at[part]).start()

    @pl.when(active)
    def _():
        g_own.start()
        bo_own.start()
        lam_own.start()
        send_g(2).start()
        for s in range(1, EXPERTS // 2):
            send_slot(s, True)
        wait_bi_plane()
        send_relay(2).start()
        for s in range(EXPERTS // 2, EXPERTS):
            send_slot(s, True)

        for step in (1, 3, 2):
            send_relay(step).wait_recv()
        lanes = inner // 128
        short = bi.shape[1] // lanes

        def unpack(f, carry):
            for c in range(lanes):
                block = jnp.concatenate(
                    [bi_all[k, f, pl.ds(c * short, short), :] for k in range(PLANES)], axis=0
                )
                high, low = split(block)
                at = pl.ds(pl.multiple_of(f * PLANES * short, PLANES * short), PLANES * short)
                bi_hi[at, pl.ds(c * 128, 128)] = high
                bi_lo[at, pl.ds(c * 128, 128)] = low
            return carry

        lax.fori_loop(0, EXPERTS, unpack, 0)

        g_own.wait()
        for step in (1, 3, 2):
            send_g(step).wait_recv()
        for k in range(PLANES):

            def to_halves(r, carry, k=k):
                at = pl.ds(pl.multiple_of(r * 64, 64), 64)
                high, low = split(g_all[k, at, :])
                into = pl.ds(pl.multiple_of(k * rows + r * 64, 64), 64)
                g_hi[into, :] = high
                g_lo[into, :] = low
                return carry

            lax.fori_loop(0, rows // 64, to_halves, 0)

        score_acc[...] = jnp.zeros_like(score_acc)
        bo_own.wait()
        lam_own.wait()

        def direction(c, carry):
            at = pl.ds(pl.multiple_of(c * chunk_rows, chunk_rows), chunk_rows)

            @pl.when(c == 0)
            def _():
                wait_bytes(bo_all.at[pl.ds(piece, chunk_rows - piece)], bo_recv.at[0])
                wait_bytes(lam_all.at[pl.ds(piece, chunk_rows - piece)], lam_recv.at[0])

            @pl.when(c > 0)
            def _():
                wait_bytes(bo_all.at[pl.ds(0, chunk_rows)], bo_recv.at[c])
                wait_bytes(lam_all.at[pl.ds(0, chunk_rows)], lam_recv.at[c])

            high, low = split(bo_all[at, :])
            bo_hi[at, :] = high
            bo_lo[at, :] = low
            first = dot(high, g_hi[...]) + dot(high, g_lo[...]) + dot(low, g_hi[...])
            high, low = split(first)
            turned = dot(high, bi_hi[...]) + dot(high, bi_lo[...]) + dot(low, bi_hi[...])
            scaled = turned / (lam_all[at, :] + DAMPING)
            score_acc[...] += jnp.sum((turned * scaled).reshape(-1, 8, inner), axis=0)
            high, low = split(scaled)
            back = dot_t(bi_hi[...], high) + dot_t(bi_lo[...], high) + dot_t(bi_hi[...], low)
            high, low = split(back)
            bt_hi[c] = high
            bt_lo[c] = low
            return carry

        lax.fori_loop(0, CHUNKS, direction, 0)

        value = jnp.sum(score_acc[...]) / (rows * PLANES * inner)
        value = jnp.where(counts[0] > 0, value, 0.0)
        lane = lax.broadcasted_iota(jnp.int32, (8, 128), 1)
        scz[m] = jnp.where(lane == query[0], value, 0.0)

        def partial(step, part):
            q = plane(step)
            cols = pl.ds(pl.multiple_of(q * rows, 128), rows)
            acc = jnp.zeros((tall, rows), F32)
            h = pl.ds(part * tall, tall)
            for c in range(CHUNKS):
                ks = pl.ds(c * chunk_rows, chunk_rows)
                ah, al = bt_hi[c, h, :], bt_lo[c, h, :]
                wh, wl = bo_hi[ks, cols], bo_lo[ks, cols]
                acc = acc + (dot(ah, wh) + dot(ah, wl) + dot(al, wh))
            return acc

        pending = []
        for part in range(parts):
            for index, step in enumerate((1, 3, 2)):
                snd[index, part] = partial(step, part)
                for c in pending:
                    c.start()
                pending = [out_copy(step, part, {1: 0, 3: 1, 2: 0}[step])]
            if part == 0:
                start_all(rounds[0])
        own[0] = partial(0, 0)
        for c in pending:
            c.start()
        wait_all(rounds[0])
        scx[x] = total(scz)
        own[1] = partial(0, 1)
        start_all(rounds[1])
        own[2] = partial(0, 2)
        wait_all(rounds[1])
        scy[y] = total(scx)
        for part in range(parts):
            out_copy(2, part, 0).wait_recv()
            finish(part, own[part] + rcv[0, part])
            if part == 0:
                start_all(rounds[2])
        wait_all(rounds[2])
        scores[...] = total(scy)

        wait_bytes(bi_all.at[0, pl.ds(0, EXPERTS - 1)], bi_send)
        send_g(2).wait_send()
        send_relay(2).wait_send()
        wait_bytes(bo_all.at[pl.ds(0, (EXPERTS - 1) * piece)], bo_send)
        wait_bytes(lam_all.at[pl.ds(0, (EXPERTS - 1) * piece)], lam_send)
        for part in range(parts):
            for step in (1, 3, 2):
                out_copy(step, part, 0).wait_send()
        for part in range(parts):
            pltpu.make_async_copy(fin.at[part], out.at[:, pl.ds(part * tall, tall)], fin_sem.at[part]).wait()

    @pl.when(jnp.logical_not(active))
    def _():
        scz[m] = jnp.zeros((8, 128), F32)
        send_g(1).start()
        send_g(3).start()
        for s in range(EXPERTS // 2):
            send_slot(s, False)
        wait_bi_plane()
        send_relay(1).start()
        send_relay(3).start()
        for s in range(EXPERTS // 2, EXPERTS):
            send_slot(s, False)
        start_all(rounds[0])
        wait_all(rounds[0])
        scx[x] = total(scz)
        wait_bytes(bi_all.at[0, pl.ds(0, EXPERTS - 1)], bi_send)
        for step in (1, 3):
            send_g(step).wait_send()
            send_relay(step).wait_send()
        wait_bytes(bo_all.at[pl.ds(0, EXPERTS * piece)], bo_send)
        wait_bytes(lam_all.at[pl.ds(0, EXPERTS * piece)], lam_send)
        start_all(rounds[1])
        wait_all(rounds[1])
        scy[y] = total(scx)
        for part in range(parts):
            out_copy(1, part, 0).wait_recv()
            out_copy(3, part, 1).wait_recv()
            finish(part, rcv[0, part] + rcv[1, part])
            if part == 0:
                start_all(rounds[2])
        wait_all(rounds[2])
        scores[...] = total(scy)
        for part in range(parts):
            pltpu.make_async_copy(fin.at[part], out.at[:, pl.ds(part * tall, tall)], fin_sem.at[part]).wait()


def shards(grads, basis_out, basis_in, eigvals, counts, slot_query):
    rows, inner = grads.shape[2:]
    experts, width, piece = basis_out.shape
    short = basis_in.shape[1]
    lanes = inner // 128
    parts = 3
    tall = inner // parts
    own_k = experts * 2 * piece
    bo = jnp.transpose(basis_out, (0, 2, 1))
    bi = basis_in.reshape(experts, short, lanes, 128).transpose(0, 2, 1, 3).reshape(experts, lanes * short, 128)
    hbm = pl.BlockSpec(memory_space=pl.ANY)
    smem = pl.BlockSpec(memory_space=pltpu.SMEM)
    dma = pltpu.SemaphoreType.DMA
    out, scores = pl.pallas_call(
        kernel,
        out_shape=(
            jax.ShapeDtypeStruct((rows, inner), F32),
            jax.ShapeDtypeStruct((8, 128), F32),
        ),
        in_specs=[hbm, hbm, hbm, hbm, smem, smem],
        out_specs=(hbm, pl.BlockSpec(memory_space=pltpu.VMEM)),
        scratch_shapes=[
            pltpu.VMEM((PLANES, rows, inner), F32),
            pltpu.VMEM((own_k, width), F32),
            pltpu.VMEM((PLANES, experts, lanes * short, 128), F32),
            pltpu.VMEM((own_k, inner), F32),
            pltpu.VMEM((PLANES * rows, inner), BF16),
            pltpu.VMEM((PLANES * rows, inner), BF16),
            pltpu.VMEM((own_k, width), BF16),
            pltpu.VMEM((own_k, width), BF16),
            pltpu.VMEM((inner, inner), BF16),
            pltpu.VMEM((inner, inner), BF16),
            pltpu.VMEM((CHUNKS, inner, own_k // CHUNKS), BF16),
            pltpu.VMEM((CHUNKS, inner, own_k // CHUNKS), BF16),
            pltpu.VMEM((3, parts, tall, rows), F32),
            pltpu.VMEM((parts, tall, rows), F32),
            pltpu.VMEM((2, parts, tall, rows), F32),
            pltpu.VMEM((parts, rows, tall), F32),
            pltpu.VMEM((8, inner), F32),
            pltpu.VMEM((4, 8, 128), F32),
            pltpu.VMEM((4, 8, 128), F32),
            pltpu.VMEM((4, 8, 128), F32),
            dma((4,)),
            dma((3,)),
            dma((3,)),
            dma(()),
            dma(()),
            dma((3,)),
            dma((3,)),
            dma(()),
            dma((CHUNKS,)),
            dma(()),
            dma((CHUNKS,)),
            dma((3, parts)),
            dma((2, parts)),
            dma((parts,)),
            dma((9,)),
            dma((9,)),
        ],
        compiler_params=pltpu.CompilerParams(has_side_effects=True, vmem_limit_bytes=66_000_000),
        name="precondition",
    )(grads[0, 0], bo, bi, eigvals, counts, slot_query[0])
    return out[None, None], scores[0, :QUERIES]


def solution(mesh):
    in_specs = (
        P(("layer", "expert"), None, "matrix", None),
        P("layer", None, ("expert", "matrix")),
        P("layer", ("expert", "matrix"), None),
        P("layer", ("expert", "matrix"), None),
        P(("layer", "expert")),
        P(("layer", "expert"), None),
    )
    out_specs = (P(("layer", "expert"), None, "matrix", None), P("layer"))
    return jax.shard_map(shards, mesh=mesh, in_specs=in_specs, out_specs=out_specs, check_vma=False)
```

```python
import functools

import jax
import jax.numpy as jnp
from jax import lax
from jax.experimental import pallas as pl
from jax.experimental.pallas import tpu as pltpu
from jax.sharding import PartitionSpec as P

MESH = pl.DeviceIdType.MESH
QUERIES = 32
SIDE = 4
PLANES = 4
EXPERTS = 16
DAMPING = 0.05
BF16 = jnp.bfloat16
F32 = jnp.float32

ORDER = [
    (0, 0), (3, 1), (1, 0), (0, 2), (2, 3), (1, 1), (0, 1), (2, 0),
    (0, 3), (3, 0), (1, 2), (3, 3), (1, 3), (2, 1), (3, 2), (2, 2),
]
OWN_CHUNKS = 2
SIDE_CHUNKS = 4
CHUNKS = OWN_CHUNKS + SIDE_CHUNKS


def split(x):
    high = x.astype(BF16)
    return high, (x - high.astype(F32)).astype(BF16)


def dot(a, b):
    return lax.dot_general(a, b, (((1,), (0,)), ((), ())), preferred_element_type=F32)


def dot_t(a, b):
    return lax.dot_general(a, b, (((1,), (1,)), ((), ())), preferred_element_type=F32)


def wait_bytes(ref, sem):
    pltpu.make_async_copy(ref, ref, sem).wait()


def three_pass(product, high, low, other_high, other_low):
    n = high.shape[0]
    both = product(jnp.concatenate([high, low], axis=0), other_high)
    return both[:n] + both[n:] + product(high, other_low)


def kernel(
    g, bo, bi, lam, counts, query, out, scores,
    g_all, bo_all, bi_raw, bi_stage, bi_all, lam_all, g_hi, g_lo, bo_hi, bo_lo, bi_hi, bi_lo,
    back_hi, back_lo, snd, score_acc, scz, scx, scy,
    loc_sem, g_send, g_recv, bi_send, bi_recv, rel_send, rel_recv,
    bo_send, bo_recv, lam_send, lam_recv, hop_send, hop_recv, out_send, out_recv, own_sem,
    sc_send, sc_recv,
):
    layer = lax.axis_index("layer")
    e = lax.axis_index("expert")
    m = lax.axis_index("matrix")
    y, x = e // SIDE, lax.rem(e, SIDE)
    active = lax.rem(m + layer, 2) == 0
    rows = g.shape[0]
    piece = bo.shape[1]
    half = piece // 2
    own_rows = EXPERTS * piece // OWN_CHUNKS
    side_rows = EXPERTS * piece // SIDE_CHUNKS
    inner = g.shape[1]
    parts = snd.shape[1]
    tall = snd.shape[2]
    lanes = inner // 128
    short = bi.shape[0]

    def plane(step):
        return lax.rem(m + step, PLANES)

    def place(d):
        return lax.rem(y + d[0], SIDE) * SIDE + lax.rem(x + d[1], SIDE)

    def remote(src, dst, send, recv, expert, matrix):
        return pltpu.make_async_remote_copy(
            src_ref=src,
            dst_ref=dst,
            send_sem=send,
            recv_sem=recv,
            device_id={"layer": layer, "expert": expert, "matrix": matrix},
            device_id_type=MESH,
        )

    bi_in = pltpu.make_async_copy(bi, bi_raw, loc_sem.at[0])
    bi_in.start()

    barrier = pltpu.get_barrier_semaphore()
    partners = [(e, plane(t)) for t in (1, 3, 2)]
    partners += [(lax.rem(e + s, EXPERTS), m) for s in range(1, EXPERTS)]
    for expert, matrix in partners:
        pl.semaphore_signal(
            barrier,
            inc=1,
            device_id={"layer": layer, "expert": expert, "matrix": matrix},
            device_id_type=MESH,
        )

    bi_in.wait()
    for to in range(EXPERTS):
        for c in range(lanes):
            bi_stage[to, pl.ds(c * short, short), :] = bi_raw[:, to, pl.ds(c * 128, 128)]

    pl.semaphore_wait(barrier, len(partners))

    steps = {1: 0, 3: 1, 2: 2}

    def send_g(step):
        return remote(g, g_all.at[m], g_send.at[steps[step]], g_recv.at[steps[step]], e, plane(step))

    g_own = pltpu.make_async_copy(g, g_all.at[m], loc_sem.at[1])
    bo_own = pltpu.make_async_copy(bo.at[e], bo_all.at[pl.ds(0, piece)], loc_sem.at[2])
    lam_own = pltpu.make_async_copy(lam.at[e], lam_all.at[pl.ds(0, piece)], loc_sem.at[3])

    def send_bi():
        for s in range(1, EXPERTS):
            to = place(ORDER[s])
            remote(bi_stage.at[to], bi_all.at[m, e], bi_send, bi_recv, to, m).start()

    def send_slot(s, is_active):
        to = place(ORDER[s])
        if is_active:
            chunk = s * OWN_CHUNKS // EXPERTS
            there = pl.ds(s * piece, piece)
            remote(bo.at[to], bo_all.at[there], bo_send, bo_recv.at[chunk], to, m).start()
            remote(lam.at[to], lam_all.at[there], lam_send, lam_recv.at[chunk], to, m).start()
        else:
            chunk = s * SIDE_CHUNKS // EXPERTS
            for which in range(2):
                mine = pl.ds(which * half, half)
                there = pl.ds((which * EXPERTS + s) * half, half)
                if s:
                    remote(bo.at[to, mine], bo_all.at[there], bo_send, hop_recv.at[0, chunk], to, m).start()
                    remote(lam.at[to, mine], lam_all.at[there], lam_send, hop_recv.at[1, chunk], to, m).start()
                else:
                    pltpu.make_async_copy(bo.at[e, mine], bo_all.at[there], loc_sem.at[which]).start()
                    pltpu.make_async_copy(lam.at[e, mine], lam_all.at[there], loc_sem.at[2 + which]).start()

    def wait_slots(chunk):
        ready = side_rows
        if chunk == 0:
            ready -= piece
            for which in range(2):
                wait_bytes(bo_all.at[pl.ds(0, half)], loc_sem.at[which])
                wait_bytes(lam_all.at[pl.ds(0, half)], loc_sem.at[2 + which])
        wait_bytes(bo_all.at[pl.ds(0, ready)], hop_recv.at[0, chunk])
        wait_bytes(lam_all.at[pl.ds(0, ready)], hop_recv.at[1, chunk])

    def hand_on(chunk):
        count = side_rows // 2
        for which, step in enumerate((1, 3)):
            here = pl.ds(which * EXPERTS * half + chunk * count, count)
            there = pl.ds(EXPERTS * piece + chunk * side_rows + which * count, count)
            at = OWN_CHUNKS + chunk
            remote(bo_all.at[here], bo_all.at[there], hop_send.at[0, which], bo_recv.at[at], e, plane(step)).start()
            remote(lam_all.at[here], lam_all.at[there], hop_send.at[1, which], lam_recv.at[at], e, plane(step)).start()

    def wait_bi_plane():
        for c in range(lanes):
            bi_all[m, e, pl.ds(c * short, short), :] = bi_stage[e, pl.ds(c * short, short), :]
        wait_bytes(bi_stage.at[pl.ds(0, EXPERTS - 1)], bi_recv)

    def send_relay(step):
        return remote(
            bi_all.at[m], bi_all.at[m], rel_send.at[steps[step]], rel_recv.at[steps[step]], e, plane(step)
        )

    def score_round(buf, me, index, step):
        copies = []
        for t in range(1, 4):
            if step == "z":
                where = (e, plane(t))
            elif step == "x":
                where = (place((0, t)), m)
            else:
                where = (place((t, 0)), m)
            at = 3 * index + t - 1
            copies.append(remote(buf.at[me], buf.at[me], sc_send.at[at], sc_recv.at[at], *where))
        return copies

    rounds = [score_round(scz, m, 0, "z"), score_round(scx, x, 1, "x"), score_round(scy, y, 2, "y")]

    def start_all(copies):
        for c in copies:
            c.start()

    def wait_all(copies):
        for c in copies:
            c.wait()

    def total(buf):
        return (buf[0] + buf[1]) + (buf[2] + buf[3])

    halves = {1: 0, 3: 1, 2: 0}

    def out_copy(step, part):
        index, to = steps[step], halves[step]
        there = out.at[to, pl.ds(part * tall, tall)]
        return remote(
            snd.at[index, part], there, out_send.at[index, part], out_recv.at[to, part], e, plane(step)
        )

    def own_copy(part):
        return pltpu.make_async_copy(snd.at[3, part], out.at[1, pl.ds(part * tall, tall)], own_sem.at[part])

    @pl.when(active)
    def _():
        g_own.start()
        bo_own.start()
        lam_own.start()
        send_g(2).start()
        send_bi()
        for s in range(1, EXPERTS):
            send_slot(s, True)
        wait_bi_plane()
        send_relay(2).start()

        g_own.wait()
        for step in (1, 3, 2):
            send_g(step).wait_recv()
        for k in range(PLANES):

            def to_halves(r, carry, k=k):
                at = pl.ds(pl.multiple_of(r * 64, 64), 64)
                high, low = split(g_all[k, at, :])
                into = pl.ds(pl.multiple_of(k * rows + r * 64, 64), 64)
                g_hi[into, :] = high
                g_lo[into, :] = low
                return carry

            lax.fori_loop(0, rows // 64, to_halves, 0)

        for step in (1, 3, 2):
            send_relay(step).wait_recv()

        def unpack(f, carry):
            for c in range(lanes):
                block = jnp.concatenate(
                    [bi_all[k, f, pl.ds(c * short, short), :] for k in range(PLANES)], axis=0
                )
                high, low = split(block)
                at = pl.ds(pl.multiple_of(f * PLANES * short, PLANES * short), PLANES * short)
                bi_hi[at, pl.ds(c * 128, 128)] = high
                bi_lo[at, pl.ds(c * 128, 128)] = low
            return carry

        lax.fori_loop(0, EXPERTS, unpack, 0)

        score_acc[...] = jnp.zeros_like(score_acc)
        bo_own.wait()
        lam_own.wait()

        def direction(start, size):
            at = pl.ds(start, size)
            columns = bo_all[at, :]
            high, low = split(columns)
            first = three_pass(dot, high, low, g_hi[...], g_lo[...])
            high, low = split(first)
            turned = three_pass(dot, high, low, bi_hi[...], bi_lo[...])
            scaled = turned / (lam_all[at, :] + DAMPING)
            score_acc[...] += jnp.sum((turned * scaled).reshape(-1, 8, inner), axis=0)
            high, low = split(scaled)
            high, low = split(three_pass(dot_t, high, low, bi_hi[...], bi_lo[...]))
            back_hi[at, :] = high
            back_lo[at, :] = low
            high, low = split(jnp.transpose(columns))
            bo_hi[:, at] = high
            bo_lo[:, at] = low

        def own_chunk(c, carry):
            @pl.when(c == 0)
            def _():
                wait_bytes(bo_all.at[pl.ds(piece, own_rows - piece)], bo_recv.at[0])
                wait_bytes(lam_all.at[pl.ds(piece, own_rows - piece)], lam_recv.at[0])

            @pl.when(c > 0)
            def _():
                wait_bytes(bo_all.at[pl.ds(0, own_rows)], bo_recv.at[c])
                wait_bytes(lam_all.at[pl.ds(0, own_rows)], lam_recv.at[c])

            direction(pl.multiple_of(c * own_rows, own_rows), own_rows)
            return carry

        def side_chunk(c, carry):
            wait_bytes(bo_all.at[pl.ds(0, side_rows)], bo_recv.at[OWN_CHUNKS + c])
            wait_bytes(lam_all.at[pl.ds(0, side_rows)], lam_recv.at[OWN_CHUNKS + c])
            direction(pl.multiple_of(EXPERTS * piece + c * side_rows, side_rows), side_rows)
            return carry

        lax.fori_loop(0, OWN_CHUNKS, own_chunk, 0)
        lax.fori_loop(0, SIDE_CHUNKS, side_chunk, 0)

        value = jnp.sum(score_acc[...]) / (rows * PLANES * inner)
        value = jnp.where(counts[0] > 0, value, 0.0)
        lane = lax.broadcasted_iota(jnp.int32, (8, 128), 1)
        scz[m] = jnp.where(lane == query[0], value, 0.0)

        def partial(step, part):
            at = pl.ds(pl.multiple_of(plane(step) * rows + part * tall, tall), tall)
            return three_pass(dot, bo_hi[at, :], bo_lo[at, :], back_hi[...], back_lo[...])

        pending = rounds[0]
        for part in range(parts):
            for index, step in enumerate((1, 3, 2)):
                snd[index, part] = partial(step, part)
                start_all(pending)
                pending = [out_copy(step, part)]
        snd[3, 0] = partial(0, 0)
        start_all(pending)
        wait_all(rounds[0])
        scx[x] = total(scz)
        snd[3, 1] = partial(0, 1)
        start_all(rounds[1])
        own_copy(0).start()
        wait_all(rounds[1])
        scy[y] = total(scx)
        for part in range(2, parts):
            snd[3, part] = partial(0, part)
            own_copy(part - 1).start()
        start_all(rounds[2])
        wait_all(rounds[2])
        scores[...] = total(scy)
        own_copy(parts - 1).start()

        wait_bytes(bi_stage.at[pl.ds(0, EXPERTS - 1)], bi_send)
        send_g(2).wait_send()
        send_relay(2).wait_send()
        wait_bytes(bo_all.at[pl.ds(0, (EXPERTS - 1) * piece)], bo_send)
        wait_bytes(lam_all.at[pl.ds(0, (EXPERTS - 1) * piece)], lam_send)
        for part in range(parts):
            for step in (1, 3, 2):
                out_copy(step, part).wait_send()
            own_copy(part).wait()
            out_copy(2, part).wait_recv()

    @pl.when(jnp.logical_not(active))
    def _():
        scz[m] = jnp.zeros((8, 128), F32)
        send_g(1).start()
        send_g(3).start()
        send_bi()
        for s in range(EXPERTS):
            send_slot(s, False)
        wait_bi_plane()
        send_relay(1).start()
        send_relay(3).start()
        for chunk in range(SIDE_CHUNKS):
            wait_slots(chunk)
            hand_on(chunk)
        start_all(rounds[0])
        wait_all(rounds[0])
        scx[x] = total(scz)
        wait_bytes(bi_stage.at[pl.ds(0, EXPERTS - 1)], bi_send)
        for which, step in enumerate((1, 3)):
            send_g(step).wait_send()
            send_relay(step).wait_send()
            wait_bytes(bo_all.at[pl.ds(0, EXPERTS * half)], hop_send.at[0, which])
            wait_bytes(lam_all.at[pl.ds(0, EXPERTS * half)], hop_send.at[1, which])
        wait_bytes(bo_all.at[pl.ds(0, (EXPERTS - 1) * piece)], bo_send)
        wait_bytes(lam_all.at[pl.ds(0, (EXPERTS - 1) * piece)], lam_send)
        start_all(rounds[1])
        wait_all(rounds[1])
        scy[y] = total(scx)
        out_copy(1, 0).wait_recv()
        start_all(rounds[2])
        wait_all(rounds[2])
        scores[...] = total(scy)
        out_copy(3, 0).wait_recv()
        for part in range(1, parts):
            out_copy(1, part).wait_recv()
            out_copy(3, part).wait_recv()


def shards(grads, basis_out, basis_in, eigvals, counts, slot_query):
    rows, inner = grads.shape[2:]
    experts, width, piece = basis_out.shape
    short = basis_in.shape[1]
    lanes = inner // 128
    parts = 4
    own_k = experts * 2 * piece
    hbm = pl.BlockSpec(memory_space=pl.ANY)
    smem = pl.BlockSpec(memory_space=pltpu.SMEM)
    dma = pltpu.SemaphoreType.DMA
    out, scores = pl.pallas_call(
        kernel,
        out_shape=(
            jax.ShapeDtypeStruct((2, rows, inner), F32),
            jax.ShapeDtypeStruct((8, 128), F32),
        ),
        in_specs=[hbm, hbm, hbm, hbm, smem, smem],
        out_specs=(hbm, pl.BlockSpec(memory_space=pltpu.VMEM)),
        scratch_shapes=[
            pltpu.VMEM((PLANES, rows, inner), F32),
            pltpu.VMEM((own_k, width), F32),
            pltpu.VMEM((short, experts, inner), F32),
            pltpu.VMEM((experts, lanes * short, 128), F32),
            pltpu.VMEM((PLANES, experts, lanes * short, 128), F32),
            pltpu.VMEM((own_k, inner), F32),
            pltpu.VMEM((PLANES * rows, inner), BF16),
            pltpu.VMEM((PLANES * rows, inner), BF16),
            pltpu.VMEM((width, own_k), BF16),
            pltpu.VMEM((width, own_k), BF16),
            pltpu.VMEM((inner, inner), BF16),
            pltpu.VMEM((inner, inner), BF16),
            pltpu.VMEM((own_k, inner), BF16),
            pltpu.VMEM((own_k, inner), BF16),
            pltpu.VMEM((4, parts, rows // parts, inner), F32),
            pltpu.VMEM((8, inner), F32),
            pltpu.VMEM((4, 8, 128), F32),
            pltpu.VMEM((4, 8, 128), F32),
            pltpu.VMEM((4, 8, 128), F32),
            dma((4,)),
            dma((3,)),
            dma((3,)),
            dma(()),
            dma(()),
            dma((3,)),
            dma((3,)),
            dma(()),
            dma((CHUNKS,)),
            dma(()),
            dma((CHUNKS,)),
            dma((2, 2)),
            dma((2, SIDE_CHUNKS)),
            dma((3, parts)),
            dma((2, parts)),
            dma((parts,)),
            dma((9,)),
            dma((9,)),
        ],
        compiler_params=pltpu.CompilerParams(
            collective_id=0, has_side_effects=True, vmem_limit_bytes=66_000_000
        ),
        name="precondition",
    )(
        grads[0, 0],
        jnp.transpose(basis_out, (0, 2, 1)),
        jnp.transpose(basis_in, (1, 0, 2)),
        eigvals,
        counts,
        slot_query[0],
    )
    live = (counts[0] > 0).astype(F32)
    return ((out[0] + out[1]) * live)[None, None], scores[0, :QUERIES]


def solution(mesh):
    in_specs = (
        P(("layer", "expert"), None, "matrix", None),
        P("layer", None, ("expert", "matrix")),
        P("layer", ("expert", "matrix"), None),
        P("layer", ("expert", "matrix"), None),
        P(("layer", "expert")),
        P(("layer", "expert"), None),
    )
    out_specs = (P(("layer", "expert"), None, "matrix", None), P("layer"))
    return jax.shard_map(shards, mesh=mesh, in_specs=in_specs, out_specs=out_specs, check_vma=False)
```

```python
import functools

import jax
import jax.numpy as jnp
from jax import lax
from jax.experimental import pallas as pl
from jax.experimental.pallas import tpu as pltpu
from jax.sharding import PartitionSpec as P

MESH = pl.DeviceIdType.MESH
QUERIES = 32
SIDE = 4
PLANES = 4
EXPERTS = 16
DAMPING = 0.05
BF16 = jnp.bfloat16
F32 = jnp.float32

ORDER = [
    (0, 0), (3, 1), (1, 0), (0, 2), (2, 3), (1, 1), (0, 1), (2, 0),
    (0, 3), (3, 0), (1, 2), (3, 3), (1, 3), (2, 1), (3, 2), (2, 2),
]
OWN_CHUNKS = 4
SIDE_CHUNKS = 4
CHUNKS = OWN_CHUNKS + SIDE_CHUNKS
EARLY = 1


def split(x):
    high = x.astype(BF16)
    return high, (x - high.astype(F32)).astype(BF16)


def dot(a, b):
    return lax.dot_general(a, b, (((1,), (0,)), ((), ())), preferred_element_type=F32)


def dot_t(a, b):
    return lax.dot_general(a, b, (((1,), (1,)), ((), ())), preferred_element_type=F32)


def wait_bytes(ref, sem):
    pltpu.make_async_copy(ref, ref, sem).wait()


def three_pass(product, high, low, other_high, other_low):
    n = high.shape[0]
    both = product(jnp.concatenate([high, low], axis=0), other_high)
    return both[:n] + both[n:] + product(high, other_low)


def kernel(
    g, bo, bi, lam, counts, query, out, scores,
    g_all, bo_all, bi_raw, bi_stage, bi_all, lam_all, g_hi, g_lo, bo_hi, bo_lo, bi_hi, bi_lo,
    back_hi, back_lo, snd, score_acc, scz, scx, scy,
    loc_sem, g_send, g_recv, bi_send, bi_recv, rel_send, rel_recv,
    bo_send, bo_recv, lam_send, lam_recv, hop_send, hop_recv, out_send, out_recv, own_sem,
    sc_send, sc_recv,
):
    layer = lax.axis_index("layer")
    e = lax.axis_index("expert")
    m = lax.axis_index("matrix")
    y, x = e // SIDE, lax.rem(e, SIDE)
    active = lax.rem(m + layer, 2) == 0
    rows = g.shape[0]
    piece = bo.shape[1]
    half = piece // 2
    own_rows = EXPERTS * piece // OWN_CHUNKS
    side_rows = EXPERTS * piece // SIDE_CHUNKS
    inner = g.shape[1]
    parts = snd.shape[1]
    tall = snd.shape[2]
    lanes = inner // 128
    short = bi.shape[0]

    def plane(step):
        return lax.rem(m + step, PLANES)

    def place(d):
        return lax.rem(y + d[0], SIDE) * SIDE + lax.rem(x + d[1], SIDE)

    def remote(src, dst, send, recv, expert, matrix):
        return pltpu.make_async_remote_copy(
            src_ref=src,
            dst_ref=dst,
            send_sem=send,
            recv_sem=recv,
            device_id={"layer": layer, "expert": expert, "matrix": matrix},
            device_id_type=MESH,
        )

    bi_in = pltpu.make_async_copy(bi, bi_raw, loc_sem.at[0])
    bi_in.start()

    barrier = pltpu.get_barrier_semaphore()
    partners = [(e, plane(t)) for t in (1, 3, 2)]
    partners += [(lax.rem(e + s, EXPERTS), m) for s in range(1, EXPERTS)]
    for expert, matrix in partners:
        pl.semaphore_signal(
            barrier,
            inc=1,
            device_id={"layer": layer, "expert": expert, "matrix": matrix},
            device_id_type=MESH,
        )

    bi_in.wait()
    for to in range(EXPERTS):
        for c in range(lanes):
            bi_stage[to, pl.ds(c * short, short), :] = bi_raw[:, to, pl.ds(c * 128, 128)]

    pl.semaphore_wait(barrier, len(partners))

    steps = {1: 0, 3: 1, 2: 2}

    def send_g(step):
        return remote(g, g_all.at[m], g_send.at[steps[step]], g_recv.at[steps[step]], e, plane(step))

    g_own = pltpu.make_async_copy(g, g_all.at[m], loc_sem.at[1])
    bo_own = pltpu.make_async_copy(bo.at[e], bo_all.at[pl.ds(0, piece)], loc_sem.at[2])
    lam_own = pltpu.make_async_copy(lam.at[e], lam_all.at[pl.ds(0, piece)], loc_sem.at[3])

    def send_bi():
        for s in range(1, EXPERTS):
            to = place(ORDER[s])
            remote(bi_stage.at[to], bi_all.at[m, e], bi_send, bi_recv, to, m).start()

    def send_slot(s, is_active):
        to = place(ORDER[s])
        if is_active:
            chunk = s * OWN_CHUNKS // EXPERTS
            there = pl.ds(s * piece, piece)
            remote(bo.at[to], bo_all.at[there], bo_send, bo_recv.at[chunk], to, m).start()
            remote(lam.at[to], lam_all.at[there], lam_send, lam_recv.at[chunk], to, m).start()
        else:
            chunk = s * SIDE_CHUNKS // EXPERTS
            for which in range(2):
                mine = pl.ds(which * half, half)
                there = pl.ds((which * EXPERTS + s) * half, half)
                if s:
                    remote(bo.at[to, mine], bo_all.at[there], bo_send, hop_recv.at[0, chunk], to, m).start()
                    remote(lam.at[to, mine], lam_all.at[there], lam_send, hop_recv.at[1, chunk], to, m).start()
                else:
                    pltpu.make_async_copy(bo.at[e, mine], bo_all.at[there], loc_sem.at[which]).start()
                    pltpu.make_async_copy(lam.at[e, mine], lam_all.at[there], loc_sem.at[2 + which]).start()

    def wait_slots(chunk):
        ready = side_rows
        if chunk == 0:
            ready -= piece
            for which in range(2):
                wait_bytes(bo_all.at[pl.ds(0, half)], loc_sem.at[which])
                wait_bytes(lam_all.at[pl.ds(0, half)], loc_sem.at[2 + which])
        wait_bytes(bo_all.at[pl.ds(0, ready)], hop_recv.at[0, chunk])
        wait_bytes(lam_all.at[pl.ds(0, ready)], hop_recv.at[1, chunk])

    def hand_on(chunk):
        count = side_rows // 2
        for which, step in enumerate((1, 3)):
            here = pl.ds(which * EXPERTS * half + chunk * count, count)
            there = pl.ds(EXPERTS * piece + chunk * side_rows + which * count, count)
            at = OWN_CHUNKS + chunk
            remote(bo_all.at[here], bo_all.at[there], hop_send.at[0, which], bo_recv.at[at], e, plane(step)).start()
            remote(lam_all.at[here], lam_all.at[there], hop_send.at[1, which], lam_recv.at[at], e, plane(step)).start()

    def wait_bi_plane():
        for c in range(lanes):
            bi_all[m, e, pl.ds(c * short, short), :] = bi_stage[e, pl.ds(c * short, short), :]
        wait_bytes(bi_stage.at[pl.ds(0, EXPERTS - 1)], bi_recv)

    def send_relay(step):
        return remote(
            bi_all.at[m], bi_all.at[m], rel_send.at[steps[step]], rel_recv.at[steps[step]], e, plane(step)
        )

    def score_round(buf, me, index, step):
        copies = []
        for t in range(1, 4):
            if step == "z":
                where = (e, plane(t))
            elif step == "x":
                where = (place((0, t)), m)
            else:
                where = (place((t, 0)), m)
            at = 3 * index + t - 1
            copies.append(remote(buf.at[me], buf.at[me], sc_send.at[at], sc_recv.at[at], *where))
        return copies

    rounds = [score_round(scz, m, 0, "z"), score_round(scx, x, 1, "x"), score_round(scy, y, 2, "y")]

    def start_all(copies):
        for c in copies:
            c.start()

    def wait_all(copies):
        for c in copies:
            c.wait()

    def total(buf):
        return (buf[0] + buf[1]) + (buf[2] + buf[3])

    halves = {1: 0, 3: 1, 2: 0}

    def out_copy(step, part):
        index, to = steps[step], halves[step]
        there = out.at[to, pl.ds(part * tall, tall)]
        return remote(
            snd.at[index, part], there, out_send.at[index, part], out_recv.at[to, part], e, plane(step)
        )

    def own_copy(part):
        return pltpu.make_async_copy(snd.at[3, part], out.at[1, pl.ds(part * tall, tall)], own_sem.at[part])

    @pl.when(active)
    def _():
        g_own.start()
        bo_own.start()
        lam_own.start()
        send_g(2).start()
        send_bi()
        for s in range(1, EARLY):
            send_slot(s, True)
        wait_bi_plane()
        send_relay(2).start()

        g_own.wait()
        for step in (1, 3):
            send_g(step).wait_recv()
        for s in range(EARLY, EXPERTS):
            send_slot(s, True)
        send_g(2).wait_recv()
        for k in range(PLANES):

            def to_halves(r, carry, k=k):
                at = pl.ds(pl.multiple_of(r * 64, 64), 64)
                high, low = split(g_all[k, at, :])
                into = pl.ds(pl.multiple_of(k * rows + r * 64, 64), 64)
                g_hi[into, :] = high
                g_lo[into, :] = low
                return carry

            lax.fori_loop(0, rows // 64, to_halves, 0)

        for step in (1, 3, 2):
            send_relay(step).wait_recv()

        def unpack(f, carry):
            for c in range(lanes):
                block = jnp.concatenate(
                    [bi_all[k, f, pl.ds(c * short, short), :] for k in range(PLANES)], axis=0
                )
                high, low = split(block)
                at = pl.ds(pl.multiple_of(f * PLANES * short, PLANES * short), PLANES * short)
                bi_hi[at, pl.ds(c * 128, 128)] = high
                bi_lo[at, pl.ds(c * 128, 128)] = low
            return carry

        lax.fori_loop(0, EXPERTS, unpack, 0)

        score_acc[...] = jnp.zeros_like(score_acc)
        bo_own.wait()
        lam_own.wait()

        def direction(start, size):
            at = pl.ds(start, size)
            columns = bo_all[at, :]
            high, low = split(columns)
            first = three_pass(dot, high, low, g_hi[...], g_lo[...])
            high, low = split(first)
            turned = three_pass(dot, high, low, bi_hi[...], bi_lo[...])
            scaled = turned / (lam_all[at, :] + DAMPING)
            score_acc[...] += jnp.sum((turned * scaled).reshape(-1, 8, inner), axis=0)
            high, low = split(scaled)
            high, low = split(three_pass(dot_t, high, low, bi_hi[...], bi_lo[...]))
            back_hi[at, :] = high
            back_lo[at, :] = low
            high, low = split(jnp.transpose(columns))
            bo_hi[:, at] = high
            bo_lo[:, at] = low

        def next_chunk(i, carry):
            side = lax.rem(i, 2)
            c = i // 2

            @pl.when(i == 0)
            def _():
                wait_bytes(bo_all.at[pl.ds(piece, own_rows - piece)], bo_recv.at[0])
                wait_bytes(lam_all.at[pl.ds(piece, own_rows - piece)], lam_recv.at[0])

            @pl.when(i > 0)
            def _():
                wait_bytes(bo_all.at[pl.ds(0, side_rows)], bo_recv.at[side * OWN_CHUNKS + c])
                wait_bytes(lam_all.at[pl.ds(0, side_rows)], lam_recv.at[side * OWN_CHUNKS + c])

            direction(pl.multiple_of(side * (EXPERTS * piece) + c * side_rows, side_rows), side_rows)
            return carry

        lax.fori_loop(0, CHUNKS, next_chunk, 0)

        value = jnp.sum(score_acc[...]) / (rows * PLANES * inner)
        value = jnp.where(counts[0] > 0, value, 0.0)
        lane = lax.broadcasted_iota(jnp.int32, (8, 128), 1)
        scz[m] = jnp.where(lane == query[0], value, 0.0)

        def partial(step, part):
            at = pl.ds(pl.multiple_of(plane(step) * rows + part * tall, tall), tall)
            return three_pass(dot, bo_hi[at, :], bo_lo[at, :], back_hi[...], back_lo[...])

        pending = rounds[0]
        for part in range(parts):
            for index, step in enumerate((1, 3, 2)):
                snd[index, part] = partial(step, part)
                start_all(pending)
                pending = [out_copy(step, part)]
        snd[3, 0] = partial(0, 0)
        start_all(pending)
        wait_all(rounds[0])
        scx[x] = total(scz)
        snd[3, 1] = partial(0, 1)
        start_all(rounds[1])
        own_copy(0).start()
        wait_all(rounds[1])
        scy[y] = total(scx)
        for part in range(2, parts):
            snd[3, part] = partial(0, part)
            own_copy(part - 1).start()
        start_all(rounds[2])
        wait_all(rounds[2])
        scores[...] = total(scy)
        own_copy(parts - 1).start()

        wait_bytes(bi_stage.at[pl.ds(0, EXPERTS - 1)], bi_send)
        send_g(2).wait_send()
        send_relay(2).wait_send()
        wait_bytes(bo_all.at[pl.ds(0, (EXPERTS - 1) * piece)], bo_send)
        wait_bytes(lam_all.at[pl.ds(0, (EXPERTS - 1) * piece)], lam_send)
        for part in range(parts):
            for step in (1, 3, 2):
                out_copy(step, part).wait_send()
            own_copy(part).wait()
            out_copy(2, part).wait_recv()

    @pl.when(jnp.logical_not(active))
    def _():
        scz[m] = jnp.zeros((8, 128), F32)
        send_g(1).start()
        send_g(3).start()
        send_bi()
        for s in range(EXPERTS):
            send_slot(s, False)
        wait_bi_plane()
        send_relay(1).start()
        send_relay(3).start()
        for chunk in range(SIDE_CHUNKS):
            wait_slots(chunk)
            hand_on(chunk)
        start_all(rounds[0])
        wait_all(rounds[0])
        scx[x] = total(scz)
        wait_bytes(bi_stage.at[pl.ds(0, EXPERTS - 1)], bi_send)
        for which, step in enumerate((1, 3)):
            send_g(step).wait_send()
            send_relay(step).wait_send()
            wait_bytes(bo_all.at[pl.ds(0, EXPERTS * half)], hop_send.at[0, which])
            wait_bytes(lam_all.at[pl.ds(0, EXPERTS * half)], hop_send.at[1, which])
        wait_bytes(bo_all.at[pl.ds(0, (EXPERTS - 1) * piece)], bo_send)
        wait_bytes(lam_all.at[pl.ds(0, (EXPERTS - 1) * piece)], lam_send)
        start_all(rounds[1])
        wait_all(rounds[1])
        scy[y] = total(scx)
        out_copy(1, 0).wait_recv()
        start_all(rounds[2])
        wait_all(rounds[2])
        scores[...] = total(scy)
        out_copy(3, 0).wait_recv()
        for part in range(1, parts):
            out_copy(1, part).wait_recv()
            out_copy(3, part).wait_recv()


def shards(grads, basis_out, basis_in, eigvals, counts, slot_query):
    rows, inner = grads.shape[2:]
    experts, width, piece = basis_out.shape
    short = basis_in.shape[1]
    lanes = inner // 128
    parts = 4
    own_k = experts * 2 * piece
    hbm = pl.BlockSpec(memory_space=pl.ANY)
    smem = pl.BlockSpec(memory_space=pltpu.SMEM)
    dma = pltpu.SemaphoreType.DMA
    out, scores = pl.pallas_call(
        kernel,
        out_shape=(
            jax.ShapeDtypeStruct((2, rows, inner), F32),
            jax.ShapeDtypeStruct((8, 128), F32),
        ),
        in_specs=[hbm, hbm, hbm, hbm, smem, smem],
        out_specs=(hbm, pl.BlockSpec(memory_space=pltpu.VMEM)),
        scratch_shapes=[
            pltpu.VMEM((PLANES, rows, inner), F32),
            pltpu.VMEM((own_k, width), F32),
            pltpu.VMEM((short, experts, inner), F32),
            pltpu.VMEM((experts, lanes * short, 128), F32),
            pltpu.VMEM((PLANES, experts, lanes * short, 128), F32),
            pltpu.VMEM((own_k, inner), F32),
            pltpu.VMEM((PLANES * rows, inner), BF16),
            pltpu.VMEM((PLANES * rows, inner), BF16),
            pltpu.VMEM((width, own_k), BF16),
            pltpu.VMEM((width, own_k), BF16),
            pltpu.VMEM((inner, inner), BF16),
            pltpu.VMEM((inner, inner), BF16),
            pltpu.VMEM((own_k, inner), BF16),
            pltpu.VMEM((own_k, inner), BF16),
            pltpu.VMEM((4, parts, rows // parts, inner), F32),
            pltpu.VMEM((8, inner), F32),
            pltpu.VMEM((4, 8, 128), F32),
            pltpu.VMEM((4, 8, 128), F32),
            pltpu.VMEM((4, 8, 128), F32),
            dma((4,)),
            dma((3,)),
            dma((3,)),
            dma(()),
            dma(()),
            dma((3,)),
            dma((3,)),
            dma(()),
            dma((CHUNKS,)),
            dma(()),
            dma((CHUNKS,)),
            dma((2, 2)),
            dma((2, SIDE_CHUNKS)),
            dma((3, parts)),
            dma((2, parts)),
            dma((parts,)),
            dma((9,)),
            dma((9,)),
        ],
        compiler_params=pltpu.CompilerParams(
            collective_id=0, has_side_effects=True, vmem_limit_bytes=66_000_000
        ),
        name="precondition",
    )(
        grads[0, 0],
        jnp.transpose(basis_out, (0, 2, 1)),
        jnp.transpose(basis_in, (1, 0, 2)),
        eigvals,
        counts,
        slot_query[0],
    )
    live = (counts[0] > 0).astype(F32)
    return ((out[0] + out[1]) * live)[None, None], scores[0, :QUERIES]


def solution(mesh):
    in_specs = (
        P(("layer", "expert"), None, "matrix", None),
        P("layer", None, ("expert", "matrix")),
        P("layer", ("expert", "matrix"), None),
        P("layer", ("expert", "matrix"), None),
        P(("layer", "expert")),
        P(("layer", "expert"), None),
    )
    out_specs = (P(("layer", "expert"), None, "matrix", None), P("layer"))
    return jax.shard_map(shards, mesh=mesh, in_specs=in_specs, out_specs=out_specs, check_vma=False)
```

```python
import functools

import jax
import jax.numpy as jnp
from jax import lax
from jax.experimental import pallas as pl
from jax.experimental.pallas import tpu as pltpu
from jax.sharding import PartitionSpec as P

MESH = pl.DeviceIdType.MESH
QUERIES = 32
SIDE = 4
PLANES = 4
EXPERTS = 16
DAMPING = 0.05
BF16 = jnp.bfloat16
F32 = jnp.float32

ORDER = [
    (0, 0), (3, 1), (1, 0), (0, 2), (2, 3), (1, 1), (0, 1), (2, 0),
    (0, 3), (3, 0), (1, 2), (3, 3), (1, 3), (2, 1), (3, 2), (2, 2),
]
OWN_CHUNKS = 4
SIDE_CHUNKS = 4
CHUNKS = OWN_CHUNKS + SIDE_CHUNKS
EARLY = 1


def split(x):
    high = x.astype(BF16)
    return high, (x - high.astype(F32)).astype(BF16)


def dot(a, b):
    return lax.dot_general(a, b, (((1,), (0,)), ((), ())), preferred_element_type=F32)


def dot_t(a, b):
    return lax.dot_general(a, b, (((1,), (1,)), ((), ())), preferred_element_type=F32)


def wait_bytes(ref, sem):
    pltpu.make_async_copy(ref, ref, sem).wait()


def three_pass(product, high, low, other_high, other_low):
    n = high.shape[0]
    both = product(jnp.concatenate([high, low], axis=0), other_high)
    return both[:n] + both[n:] + product(high, other_low)


def kernel(
    g, bo, bi, lam, counts, query, out, scores,
    g_all, bo_all, bi_raw, bi_stage, bi_all, lam_all, g_hi, g_lo, bo_hi, bo_lo, bi_hi, bi_lo,
    back_hi, back_lo, snd, score_acc, scz, scx, scy,
    loc_sem, g_send, g_recv, bi_send, bi_recv, rel_send, rel_recv,
    bo_send, bo_recv, lam_send, lam_recv, hop_send, hop_recv, out_send, out_recv, own_sem,
    sc_send, sc_recv,
):
    layer = lax.axis_index("layer")
    e = lax.axis_index("expert")
    m = lax.axis_index("matrix")
    y, x = e // SIDE, lax.rem(e, SIDE)
    active = lax.rem(m + layer, 2) == 0
    rows = g.shape[0]
    piece = bo.shape[1]
    half = piece // 2
    own_rows = EXPERTS * piece // OWN_CHUNKS
    side_rows = EXPERTS * piece // SIDE_CHUNKS
    inner = g.shape[1]
    parts = snd.shape[1]
    tall = snd.shape[2]
    lanes = inner // 128
    short = bi.shape[0]

    def plane(step):
        return lax.rem(m + step, PLANES)

    def place(d):
        return lax.rem(y + d[0], SIDE) * SIDE + lax.rem(x + d[1], SIDE)

    def remote(src, dst, send, recv, expert, matrix):
        return pltpu.make_async_remote_copy(
            src_ref=src,
            dst_ref=dst,
            send_sem=send,
            recv_sem=recv,
            device_id={"layer": layer, "expert": expert, "matrix": matrix},
            device_id_type=MESH,
        )

    bi_in = pltpu.make_async_copy(bi, bi_raw, loc_sem.at[0])
    bi_in.start()

    barrier = pltpu.get_barrier_semaphore()
    partners = [(e, plane(t)) for t in (1, 3, 2)]
    partners += [(lax.rem(e + s, EXPERTS), m) for s in range(1, EXPERTS)]
    for expert, matrix in partners:
        pl.semaphore_signal(
            barrier,
            inc=1,
            device_id={"layer": layer, "expert": expert, "matrix": matrix},
            device_id_type=MESH,
        )

    pl.semaphore_wait(barrier, len(partners))

    steps = {1: 0, 3: 1, 2: 2}

    def send_g(step):
        return remote(g, g_all.at[m], g_send.at[steps[step]], g_recv.at[steps[step]], e, plane(step))

    g_own = pltpu.make_async_copy(g, g_all.at[m], loc_sem.at[1])

    @pl.when(active)
    def _():
        g_own.start()
        send_g(2).start()

    @pl.when(jnp.logical_not(active))
    def _():
        send_g(1).start()
        send_g(3).start()

    bi_in.wait()
    for to in range(EXPERTS):
        for c in range(lanes):
            bi_stage[to, pl.ds(c * short, short), :] = bi_raw[:, to, pl.ds(c * 128, 128)]

    bo_own = pltpu.make_async_copy(bo.at[e], bo_all.at[pl.ds(0, piece)], loc_sem.at[2])
    lam_own = pltpu.make_async_copy(lam.at[e], lam_all.at[pl.ds(0, piece)], loc_sem.at[3])

    def send_bi():
        for s in range(1, EXPERTS):
            to = place(ORDER[s])
            remote(bi_stage.at[to], bi_all.at[m, e], bi_send, bi_recv, to, m).start()

    def send_slot(s, is_active):
        to = place(ORDER[s])
        if is_active:
            chunk = s * OWN_CHUNKS // EXPERTS
            there = pl.ds(s * piece, piece)
            remote(bo.at[to], bo_all.at[there], bo_send, bo_recv.at[chunk], to, m).start()
            remote(lam.at[to], lam_all.at[there], lam_send, lam_recv.at[chunk], to, m).start()
        else:
            chunk = s * SIDE_CHUNKS // EXPERTS
            for which in range(2):
                mine = pl.ds(which * half, half)
                there = pl.ds((which * EXPERTS + s) * half, half)
                if s:
                    remote(bo.at[to, mine], bo_all.at[there], bo_send, hop_recv.at[0, chunk], to, m).start()
                    remote(lam.at[to, mine], lam_all.at[there], lam_send, hop_recv.at[1, chunk], to, m).start()
                else:
                    pltpu.make_async_copy(bo.at[e, mine], bo_all.at[there], loc_sem.at[which]).start()
                    pltpu.make_async_copy(lam.at[e, mine], lam_all.at[there], loc_sem.at[2 + which]).start()

    def wait_slots(chunk):
        ready = side_rows
        if chunk == 0:
            ready -= piece
            for which in range(2):
                wait_bytes(bo_all.at[pl.ds(0, half)], loc_sem.at[which])
                wait_bytes(lam_all.at[pl.ds(0, half)], loc_sem.at[2 + which])
        wait_bytes(bo_all.at[pl.ds(0, ready)], hop_recv.at[0, chunk])
        wait_bytes(lam_all.at[pl.ds(0, ready)], hop_recv.at[1, chunk])

    def hand_on(chunk):
        count = side_rows // 2
        for which, step in enumerate((1, 3)):
            here = pl.ds(which * EXPERTS * half + chunk * count, count)
            there = pl.ds(EXPERTS * piece + chunk * side_rows + which * count, count)
            at = OWN_CHUNKS + chunk
            remote(bo_all.at[here], bo_all.at[there], hop_send.at[0, which], bo_recv.at[at], e, plane(step)).start()
            remote(lam_all.at[here], lam_all.at[there], hop_send.at[1, which], lam_recv.at[at], e, plane(step)).start()

    def wait_bi_plane():
        for c in range(lanes):
            bi_all[m, e, pl.ds(c * short, short), :] = bi_stage[e, pl.ds(c * short, short), :]
        wait_bytes(bi_stage.at[pl.ds(0, EXPERTS - 1)], bi_recv)

    def send_relay(step):
        return remote(
            bi_all.at[m], bi_all.at[m], rel_send.at[steps[step]], rel_recv.at[steps[step]], e, plane(step)
        )

    def score_round(buf, me, index, step):
        copies = []
        for t in range(1, 4):
            if step == "z":
                where = (e, plane(t))
            elif step == "x":
                where = (place((0, t)), m)
            else:
                where = (place((t, 0)), m)
            at = 3 * index + t - 1
            copies.append(remote(buf.at[me], buf.at[me], sc_send.at[at], sc_recv.at[at], *where))
        return copies

    rounds = [score_round(scz, m, 0, "z"), score_round(scx, x, 1, "x"), score_round(scy, y, 2, "y")]

    def start_all(copies):
        for c in copies:
            c.start()

    def wait_all(copies):
        for c in copies:
            c.wait()

    def total(buf):
        return (buf[0] + buf[1]) + (buf[2] + buf[3])

    halves = {1: 0, 3: 1, 2: 0}

    def out_copy(step, part):
        index, to = steps[step], halves[step]
        there = out.at[to, pl.ds(part * tall, tall)]
        return remote(
            snd.at[index, part], there, out_send.at[index, part], out_recv.at[to, part], e, plane(step)
        )

    def own_copy(part):
        return pltpu.make_async_copy(snd.at[3, part], out.at[1, pl.ds(part * tall, tall)], own_sem.at[part])

    @pl.when(active)
    def _():
        bo_own.start()
        lam_own.start()
        send_bi()
        for s in range(1, EARLY):
            send_slot(s, True)
        wait_bi_plane()
        send_relay(2).start()

        g_own.wait()
        for step in (1, 3):
            send_g(step).wait_recv()
        for s in range(EARLY, EXPERTS):
            send_slot(s, True)
        send_g(2).wait_recv()
        for k in range(PLANES):

            def to_halves(r, carry, k=k):
                at = pl.ds(pl.multiple_of(r * 64, 64), 64)
                high, low = split(g_all[k, at, :])
                into = pl.ds(pl.multiple_of(k * rows + r * 64, 64), 64)
                g_hi[into, :] = high
                g_lo[into, :] = low
                return carry

            lax.fori_loop(0, rows // 64, to_halves, 0)

        for step in (1, 3, 2):
            send_relay(step).wait_recv()

        def unpack(f, carry):
            for c in range(lanes):
                block = jnp.concatenate(
                    [bi_all[k, f, pl.ds(c * short, short), :] for k in range(PLANES)], axis=0
                )
                high, low = split(block)
                at = pl.ds(pl.multiple_of(f * PLANES * short, PLANES * short), PLANES * short)
                bi_hi[at, pl.ds(c * 128, 128)] = high
                bi_lo[at, pl.ds(c * 128, 128)] = low
            return carry

        lax.fori_loop(0, EXPERTS, unpack, 0)

        score_acc[...] = jnp.zeros_like(score_acc)
        bo_own.wait()
        lam_own.wait()

        def direction(start, size):
            at = pl.ds(start, size)
            columns = bo_all[at, :]
            high, low = split(columns)
            first = three_pass(dot, high, low, g_hi[...], g_lo[...])
            high, low = split(first)
            turned = three_pass(dot, high, low, bi_hi[...], bi_lo[...])
            scaled = turned / (lam_all[at, :] + DAMPING)
            score_acc[...] += jnp.sum((turned * scaled).reshape(-1, 8, inner), axis=0)
            high, low = split(scaled)
            high, low = split(three_pass(dot_t, high, low, bi_hi[...], bi_lo[...]))
            back_hi[at, :] = high
            back_lo[at, :] = low
            high, low = split(jnp.transpose(columns))
            bo_hi[:, at] = high
            bo_lo[:, at] = low

        def next_chunk(i, carry):
            side = lax.rem(i + 1, 2)
            c = i // 2

            @pl.when(i == 1)
            def _():
                wait_bytes(bo_all.at[pl.ds(piece, own_rows - piece)], bo_recv.at[0])
                wait_bytes(lam_all.at[pl.ds(piece, own_rows - piece)], lam_recv.at[0])

            @pl.when(i != 1)
            def _():
                wait_bytes(bo_all.at[pl.ds(0, side_rows)], bo_recv.at[side * OWN_CHUNKS + c])
                wait_bytes(lam_all.at[pl.ds(0, side_rows)], lam_recv.at[side * OWN_CHUNKS + c])

            direction(pl.multiple_of(side * (EXPERTS * piece) + c * side_rows, side_rows), side_rows)
            return carry

        lax.fori_loop(0, CHUNKS, next_chunk, 0)

        value = jnp.sum(score_acc[...]) / (rows * PLANES * inner)
        value = jnp.where(counts[0] > 0, value, 0.0)
        lane = lax.broadcasted_iota(jnp.int32, (8, 128), 1)
        scz[m] = jnp.where(lane == query[0], value, 0.0)

        def partial(step, part):
            at = pl.ds(pl.multiple_of(plane(step) * rows + part * tall, tall), tall)
            return three_pass(dot, bo_hi[at, :], bo_lo[at, :], back_hi[...], back_lo[...])

        pending = rounds[0]
        for part in range(parts):
            for index, step in enumerate((1, 3, 2)):
                snd[index, part] = partial(step, part)
                start_all(pending)
                pending = [out_copy(step, part)]
        snd[3, 0] = partial(0, 0)
        start_all(pending)
        wait_all(rounds[0])
        scx[x] = total(scz)
        snd[3, 1] = partial(0, 1)
        start_all(rounds[1])
        own_copy(0).start()
        wait_all(rounds[1])
        scy[y] = total(scx)
        for part in range(2, parts):
            snd[3, part] = partial(0, part)
            own_copy(part - 1).start()
        start_all(rounds[2])
        wait_all(rounds[2])
        scores[...] = total(scy)
        own_copy(parts - 1).start()

        wait_bytes(bi_stage.at[pl.ds(0, EXPERTS - 1)], bi_send)
        send_g(2).wait_send()
        send_relay(2).wait_send()
        wait_bytes(bo_all.at[pl.ds(0, (EXPERTS - 1) * piece)], bo_send)
        wait_bytes(lam_all.at[pl.ds(0, (EXPERTS - 1) * piece)], lam_send)
        for part in range(parts):
            for step in (1, 3, 2):
                out_copy(step, part).wait_send()
            own_copy(part).wait()
            out_copy(2, part).wait_recv()

    @pl.when(jnp.logical_not(active))
    def _():
        scz[m] = jnp.zeros((8, 128), F32)
        send_bi()
        for s in range(EXPERTS):
            send_slot(s, False)
        wait_bi_plane()
        send_relay(1).start()
        send_relay(3).start()
        for chunk in range(SIDE_CHUNKS):
            wait_slots(chunk)
            hand_on(chunk)
        start_all(rounds[0])
        wait_all(rounds[0])
        scx[x] = total(scz)
        wait_bytes(bi_stage.at[pl.ds(0, EXPERTS - 1)], bi_send)
        for which, step in enumerate((1, 3)):
            send_g(step).wait_send()
            send_relay(step).wait_send()
            wait_bytes(bo_all.at[pl.ds(0, EXPERTS * half)], hop_send.at[0, which])
            wait_bytes(lam_all.at[pl.ds(0, EXPERTS * half)], hop_send.at[1, which])
        wait_bytes(bo_all.at[pl.ds(0, (EXPERTS - 1) * piece)], bo_send)
        wait_bytes(lam_all.at[pl.ds(0, (EXPERTS - 1) * piece)], lam_send)
        start_all(rounds[1])
        wait_all(rounds[1])
        scy[y] = total(scx)
        out_copy(1, 0).wait_recv()
        start_all(rounds[2])
        wait_all(rounds[2])
        scores[...] = total(scy)
        out_copy(3, 0).wait_recv()
        for part in range(1, parts):
            out_copy(1, part).wait_recv()
            out_copy(3, part).wait_recv()


def shards(grads, basis_out, basis_in, eigvals, counts, slot_query):
    rows, inner = grads.shape[2:]
    experts, width, piece = basis_out.shape
    short = basis_in.shape[1]
    lanes = inner // 128
    parts = 4
    own_k = experts * 2 * piece
    hbm = pl.BlockSpec(memory_space=pl.ANY)
    smem = pl.BlockSpec(memory_space=pltpu.SMEM)
    dma = pltpu.SemaphoreType.DMA
    out, scores = pl.pallas_call(
        kernel,
        out_shape=(
            jax.ShapeDtypeStruct((2, rows, inner), F32),
            jax.ShapeDtypeStruct((8, 128), F32),
        ),
        in_specs=[hbm, hbm, hbm, hbm, smem, smem],
        out_specs=(hbm, pl.BlockSpec(memory_space=pltpu.VMEM)),
        scratch_shapes=[
            pltpu.VMEM((PLANES, rows, inner), F32),
            pltpu.VMEM((own_k, width), F32),
            pltpu.VMEM((short, experts, inner), F32),
            pltpu.VMEM((experts, lanes * short, 128), F32),
            pltpu.VMEM((PLANES, experts, lanes * short, 128), F32),
            pltpu.VMEM((own_k, inner), F32),
            pltpu.VMEM((PLANES * rows, inner), BF16),
            pltpu.VMEM((PLANES * rows, inner), BF16),
            pltpu.VMEM((width, own_k), BF16),
            pltpu.VMEM((width, own_k), BF16),
            pltpu.VMEM((inner, inner), BF16),
            pltpu.VMEM((inner, inner), BF16),
            pltpu.VMEM((own_k, inner), BF16),
            pltpu.VMEM((own_k, inner), BF16),
            pltpu.VMEM((4, parts, rows // parts, inner), F32),
            pltpu.VMEM((8, inner), F32),
            pltpu.VMEM((4, 8, 128), F32),
            pltpu.VMEM((4, 8, 128), F32),
            pltpu.VMEM((4, 8, 128), F32),
            dma((4,)),
            dma((3,)),
            dma((3,)),
            dma(()),
            dma(()),
            dma((3,)),
            dma((3,)),
            dma(()),
            dma((CHUNKS,)),
            dma(()),
            dma((CHUNKS,)),
            dma((2, 2)),
            dma((2, SIDE_CHUNKS)),
            dma((3, parts)),
            dma((2, parts)),
            dma((parts,)),
            dma((9,)),
            dma((9,)),
        ],
        compiler_params=pltpu.CompilerParams(
            collective_id=0, has_side_effects=True, vmem_limit_bytes=66_000_000
        ),
        name="precondition",
    )(
        grads[0, 0],
        jnp.transpose(basis_out, (0, 2, 1)),
        jnp.transpose(basis_in, (1, 0, 2)),
        eigvals,
        counts,
        slot_query[0],
    )
    live = (counts[0] > 0).astype(F32)
    return ((out[0] + out[1]) * live)[None, None], scores[0, :QUERIES]


def solution(mesh):
    in_specs = (
        P(("layer", "expert"), None, "matrix", None),
        P("layer", None, ("expert", "matrix")),
        P("layer", ("expert", "matrix"), None),
        P("layer", ("expert", "matrix"), None),
        P(("layer", "expert")),
        P(("layer", "expert"), None),
    )
    out_specs = (P(("layer", "expert"), None, "matrix", None), P("layer"))
    return jax.shard_map(shards, mesh=mesh, in_specs=in_specs, out_specs=out_specs, check_vma=False)
```

```python
import functools

import jax
import jax.numpy as jnp
from jax import lax
from jax.experimental import pallas as pl
from jax.experimental.pallas import tpu as pltpu
from jax.sharding import PartitionSpec as P

MESH = pl.DeviceIdType.MESH
QUERIES = 32
SIDE = 4
PLANES = 4
EXPERTS = 16
DAMPING = 0.05
BF16 = jnp.bfloat16
F32 = jnp.float32

ORDER = [
    (0, 0), (3, 1), (1, 0), (0, 2), (2, 3), (1, 1), (0, 1), (2, 0),
    (0, 3), (3, 0), (1, 2), (3, 3), (1, 3), (2, 1), (3, 2), (2, 2),
]
OWN_CHUNKS = 4
SIDE_CHUNKS = 4
CHUNKS = OWN_CHUNKS + SIDE_CHUNKS
HOPS = 8
EARLY = 1


def split(x):
    high = x.astype(BF16)
    return high, (x - high.astype(F32)).astype(BF16)


def dot(a, b):
    return lax.dot_general(a, b, (((1,), (0,)), ((), ())), preferred_element_type=F32)


def wait_bytes(ref, sem):
    pltpu.make_async_copy(ref, ref, sem).wait()


def three_pass(product, high, low, other_high, other_low):
    n = high.shape[0]
    both = product(jnp.concatenate([high, low], axis=0), other_high)
    return both[:n] + both[n:] + product(high, other_low)


def kernel(
    g, bo, bi, lam, counts, query, out, scores,
    g_all, bo_all, bi_raw, bi_stage, bi_all, lam_all, g_hi, g_lo, bo_hi, bo_lo, bi_hi, bi_lo, bit_hi, bit_lo,
    back_hi, back_lo, snd, score_acc, scz, scx, scy,
    loc_sem, g_send, g_recv, bi_send, bi_recv, rel_send, rel_recv,
    bo_send, bo_recv, lam_send, lam_recv, hop_send, hop_recv, out_send, out_recv, own_sem,
    sc_send, sc_recv,
):
    layer = lax.axis_index("layer")
    e = lax.axis_index("expert")
    m = lax.axis_index("matrix")
    y, x = e // SIDE, lax.rem(e, SIDE)
    active = lax.rem(m + layer, 2) == 0
    rows = g.shape[0]
    piece = bo.shape[1]
    half = piece // 2
    own_rows = EXPERTS * piece // OWN_CHUNKS
    side_rows = EXPERTS * piece // SIDE_CHUNKS
    inner = g.shape[1]
    parts = snd.shape[1]
    tall = snd.shape[2]
    lanes = inner // 128
    short = bi.shape[0]

    def plane(step):
        return lax.rem(m + step, PLANES)

    def place(d):
        return lax.rem(y + d[0], SIDE) * SIDE + lax.rem(x + d[1], SIDE)

    def remote(src, dst, send, recv, expert, matrix):
        return pltpu.make_async_remote_copy(
            src_ref=src,
            dst_ref=dst,
            send_sem=send,
            recv_sem=recv,
            device_id={"layer": layer, "expert": expert, "matrix": matrix},
            device_id_type=MESH,
        )

    bi_in = pltpu.make_async_copy(bi, bi_raw, loc_sem.at[0])
    bi_in.start()

    barrier = pltpu.get_barrier_semaphore()
    partners = [(e, plane(t)) for t in (1, 3, 2)]
    partners += [(lax.rem(e + s, EXPERTS), m) for s in range(1, EXPERTS)]
    for expert, matrix in partners:
        pl.semaphore_signal(
            barrier,
            inc=1,
            device_id={"layer": layer, "expert": expert, "matrix": matrix},
            device_id_type=MESH,
        )

    pl.semaphore_wait(barrier, len(partners))

    steps = {1: 0, 3: 1, 2: 2}

    def send_g(step):
        return remote(g, g_all.at[m], g_send.at[steps[step]], g_recv.at[steps[step]], e, plane(step))

    g_own = pltpu.make_async_copy(g, g_all.at[m], loc_sem.at[1])

    @pl.when(active)
    def _():
        g_own.start()
        send_g(2).start()

    @pl.when(jnp.logical_not(active))
    def _():
        send_g(1).start()
        send_g(3).start()

    bi_in.wait()
    for to in range(EXPERTS):
        for c in range(lanes):
            bi_stage[to, pl.ds(c * short, short), :] = bi_raw[:, to, pl.ds(c * 128, 128)]

    bo_own = pltpu.make_async_copy(bo.at[e], bo_all.at[pl.ds(0, piece)], loc_sem.at[2])
    lam_own = pltpu.make_async_copy(lam.at[e], lam_all.at[pl.ds(0, piece)], loc_sem.at[3])

    def send_bi():
        for s in range(1, EXPERTS):
            to = place(ORDER[s])
            remote(bi_stage.at[to], bi_all.at[m, e], bi_send, bi_recv, to, m).start()

    def send_slot(s, is_active):
        to = place(ORDER[s])
        if is_active:
            chunk = s * OWN_CHUNKS // EXPERTS
            there = pl.ds(s * piece, piece)
            remote(bo.at[to], bo_all.at[there], bo_send, bo_recv.at[chunk], to, m).start()
            remote(lam.at[to], lam_all.at[there], lam_send, lam_recv.at[chunk], to, m).start()
        else:
            group = s * HOPS // EXPERTS
            for which in range(2):
                mine = pl.ds(which * half, half)
                there = pl.ds((which * EXPERTS + s) * half, half)
                if s:
                    remote(bo.at[to, mine], bo_all.at[there], bo_send, hop_recv.at[0, group], to, m).start()
                    remote(lam.at[to, mine], lam_all.at[there], lam_send, hop_recv.at[1, group], to, m).start()
                else:
                    pltpu.make_async_copy(bo.at[e, mine], bo_all.at[there], loc_sem.at[which]).start()
                    pltpu.make_async_copy(lam.at[e, mine], lam_all.at[there], loc_sem.at[2 + which]).start()

    hop_rows = EXPERTS * half // HOPS

    def wait_slots(group):
        ready = 2 * hop_rows
        if group == 0:
            ready -= piece
            for which in range(2):
                wait_bytes(bo_all.at[pl.ds(0, half)], loc_sem.at[which])
                wait_bytes(lam_all.at[pl.ds(0, half)], loc_sem.at[2 + which])
        wait_bytes(bo_all.at[pl.ds(0, ready)], hop_recv.at[0, group])
        wait_bytes(lam_all.at[pl.ds(0, ready)], hop_recv.at[1, group])

    def hand_on(group):
        chunk, place_in = divmod(group, HOPS // SIDE_CHUNKS)
        at = OWN_CHUNKS + chunk
        for which, step in enumerate((1, 3)):
            here = pl.ds(which * EXPERTS * half + group * hop_rows, hop_rows)
            start = EXPERTS * piece + chunk * side_rows + which * (side_rows // 2) + place_in * hop_rows
            there = pl.ds(start, hop_rows)
            remote(bo_all.at[here], bo_all.at[there], hop_send.at[0, which], bo_recv.at[at], e, plane(step)).start()
            remote(lam_all.at[here], lam_all.at[there], hop_send.at[1, which], lam_recv.at[at], e, plane(step)).start()

    def wait_bi_plane():
        for c in range(lanes):
            bi_all[m, e, pl.ds(c * short, short), :] = bi_stage[e, pl.ds(c * short, short), :]
        wait_bytes(bi_stage.at[pl.ds(0, EXPERTS - 1)], bi_recv)

    def send_relay(step):
        return remote(
            bi_all.at[m], bi_all.at[m], rel_send.at[steps[step]], rel_recv.at[steps[step]], e, plane(step)
        )

    def score_round(buf, me, index, step):
        copies = []
        for t in range(1, 4):
            if step == "z":
                where = (e, plane(t))
            elif step == "x":
                where = (place((0, t)), m)
            else:
                where = (place((t, 0)), m)
            at = 3 * index + t - 1
            copies.append(remote(buf.at[me], buf.at[me], sc_send.at[at], sc_recv.at[at], *where))
        return copies

    rounds = [score_round(scz, m, 0, "z"), score_round(scx, x, 1, "x"), score_round(scy, y, 2, "y")]

    def start_all(copies):
        for c in copies:
            c.start()

    def wait_all(copies):
        for c in copies:
            c.wait()

    def total(buf):
        return (buf[0] + buf[1]) + (buf[2] + buf[3])

    halves = {1: 0, 3: 1, 2: 0}

    def out_copy(step, part):
        index, to = steps[step], halves[step]
        there = out.at[to, pl.ds(part * tall, tall)]
        return remote(
            snd.at[index, part], there, out_send.at[index, part], out_recv.at[to, part], e, plane(step)
        )

    def own_copy(part):
        return pltpu.make_async_copy(snd.at[3, part], out.at[1, pl.ds(part * tall, tall)], own_sem.at[part])

    @pl.when(active)
    def _():
        bo_own.start()
        lam_own.start()
        send_bi()
        for s in range(1, EARLY):
            send_slot(s, True)
        wait_bi_plane()
        send_relay(2).start()

        g_own.wait()
        for step in (1, 3):
            send_g(step).wait_recv()
        for s in range(EARLY, EXPERTS):
            send_slot(s, True)
        send_g(2).wait_recv()
        for k in range(PLANES):

            def to_halves(r, carry, k=k):
                at = pl.ds(pl.multiple_of(r * 64, 64), 64)
                high, low = split(g_all[k, at, :])
                into = pl.ds(pl.multiple_of(k * rows + r * 64, 64), 64)
                g_hi[into, :] = high
                g_lo[into, :] = low
                return carry

            lax.fori_loop(0, rows // 64, to_halves, 0)

        for step in (1, 3, 2):
            send_relay(step).wait_recv()

        def unpack(f, carry):
            for c in range(lanes):
                block = jnp.concatenate(
                    [bi_all[k, f, pl.ds(c * short, short), :] for k in range(PLANES)], axis=0
                )
                high, low = split(block)
                at = pl.ds(pl.multiple_of(f * PLANES * short, PLANES * short), PLANES * short)
                bi_hi[at, pl.ds(c * 128, 128)] = high
                bi_lo[at, pl.ds(c * 128, 128)] = low
            return carry

        lax.fori_loop(0, EXPERTS, unpack, 0)
        bit_hi[...] = jnp.transpose(bi_hi[...])
        bit_lo[...] = jnp.transpose(bi_lo[...])

        score_acc[...] = jnp.zeros_like(score_acc)
        bo_own.wait()
        lam_own.wait()

        def direction(start, size):
            at = pl.ds(start, size)
            columns = bo_all[at, :]
            high, low = split(columns)
            first = three_pass(dot, high, low, g_hi[...], g_lo[...])
            high, low = split(first)
            turned = three_pass(dot, high, low, bi_hi[...], bi_lo[...])
            scaled = turned / (lam_all[at, :] + DAMPING)
            score_acc[...] += jnp.sum((turned * scaled).reshape(-1, 8, inner), axis=0)
            high, low = split(scaled)
            high, low = split(three_pass(dot, high, low, bit_hi[...], bit_lo[...]))
            back_hi[at, :] = high
            back_lo[at, :] = low
            high, low = split(jnp.transpose(columns))
            bo_hi[:, at] = high
            bo_lo[:, at] = low

        def next_chunk(i, carry):
            side = lax.rem(i + 1, 2)
            c = i // 2

            @pl.when(i == 1)
            def _():
                wait_bytes(bo_all.at[pl.ds(piece, own_rows - piece)], bo_recv.at[0])
                wait_bytes(lam_all.at[pl.ds(piece, own_rows - piece)], lam_recv.at[0])

            @pl.when(i != 1)
            def _():
                wait_bytes(bo_all.at[pl.ds(0, side_rows)], bo_recv.at[side * OWN_CHUNKS + c])
                wait_bytes(lam_all.at[pl.ds(0, side_rows)], lam_recv.at[side * OWN_CHUNKS + c])

            direction(pl.multiple_of(side * (EXPERTS * piece) + c * side_rows, side_rows), side_rows)
            return carry

        lax.fori_loop(0, CHUNKS, next_chunk, 0)

        value = jnp.sum(score_acc[...]) / (rows * PLANES * inner)
        value = jnp.where(counts[0] > 0, value, 0.0)
        lane = lax.broadcasted_iota(jnp.int32, (8, 128), 1)
        scz[m] = jnp.where(lane == query[0], value, 0.0)

        def partial(step, part):
            at = pl.ds(pl.multiple_of(plane(step) * rows + part * tall, tall), tall)
            return three_pass(dot, bo_hi[at, :], bo_lo[at, :], back_hi[...], back_lo[...])

        pending = rounds[0]
        for part in range(parts):
            for index, step in enumerate((1, 3, 2)):
                snd[index, part] = partial(step, part)
                start_all(pending)
                pending = [out_copy(step, part)]
        snd[3, 0] = partial(0, 0)
        start_all(pending)
        wait_all(rounds[0])
        scx[x] = total(scz)
        snd[3, 1] = partial(0, 1)
        start_all(rounds[1])
        own_copy(0).start()
        wait_all(rounds[1])
        scy[y] = total(scx)
        for part in range(2, parts):
            snd[3, part] = partial(0, part)
            own_copy(part - 1).start()
        start_all(rounds[2])
        wait_all(rounds[2])
        scores[...] = total(scy)[0:1, :QUERIES]
        own_copy(parts - 1).start()

        wait_bytes(bi_stage.at[pl.ds(0, EXPERTS - 1)], bi_send)
        send_g(2).wait_send()
        send_relay(2).wait_send()
        wait_bytes(bo_all.at[pl.ds(0, (EXPERTS - 1) * piece)], bo_send)
        wait_bytes(lam_all.at[pl.ds(0, (EXPERTS - 1) * piece)], lam_send)
        for part in range(parts):
            for step in (1, 3, 2):
                out_copy(step, part).wait_send()
            own_copy(part).wait()
            out_copy(2, part).wait_recv()

    @pl.when(jnp.logical_not(active))
    def _():
        scz[m] = jnp.zeros((8, 128), F32)
        send_bi()
        for s in range(EXPERTS):
            send_slot(s, False)
        wait_bi_plane()
        send_relay(1).start()
        send_relay(3).start()
        for group in range(HOPS):
            wait_slots(group)
            hand_on(group)
        start_all(rounds[0])
        wait_all(rounds[0])
        scx[x] = total(scz)
        wait_bytes(bi_stage.at[pl.ds(0, EXPERTS - 1)], bi_send)
        for which, step in enumerate((1, 3)):
            send_g(step).wait_send()
            send_relay(step).wait_send()
            wait_bytes(bo_all.at[pl.ds(0, EXPERTS * half)], hop_send.at[0, which])
            wait_bytes(lam_all.at[pl.ds(0, EXPERTS * half)], hop_send.at[1, which])
        wait_bytes(bo_all.at[pl.ds(0, (EXPERTS - 1) * piece)], bo_send)
        wait_bytes(lam_all.at[pl.ds(0, (EXPERTS - 1) * piece)], lam_send)
        start_all(rounds[1])
        wait_all(rounds[1])
        scy[y] = total(scx)
        out_copy(1, 0).wait_recv()
        start_all(rounds[2])
        wait_all(rounds[2])
        scores[...] = total(scy)[0:1, :QUERIES]
        out_copy(3, 0).wait_recv()
        for part in range(1, parts):
            out_copy(1, part).wait_recv()
            out_copy(3, part).wait_recv()


def shards(grads, basis_out, basis_in, eigvals, counts, slot_query):
    rows, inner = grads.shape[2:]
    experts, width, piece = basis_out.shape
    short = basis_in.shape[1]
    lanes = inner // 128
    parts = 4
    own_k = experts * 2 * piece
    hbm = pl.BlockSpec(memory_space=pl.ANY)
    smem = pl.BlockSpec(memory_space=pltpu.SMEM)
    dma = pltpu.SemaphoreType.DMA
    out, scores = pl.pallas_call(
        kernel,
        out_shape=(
            jax.ShapeDtypeStruct((2, rows, inner), F32),
            jax.ShapeDtypeStruct((1, QUERIES), F32),
        ),
        in_specs=[hbm, hbm, hbm, hbm, smem, smem],
        out_specs=(hbm, pl.BlockSpec(memory_space=pltpu.VMEM)),
        scratch_shapes=[
            pltpu.VMEM((PLANES, rows, inner), F32),
            pltpu.VMEM((own_k, width), F32),
            pltpu.VMEM((short, experts, inner), F32),
            pltpu.VMEM((experts, lanes * short, 128), F32),
            pltpu.VMEM((PLANES, experts, lanes * short, 128), F32),
            pltpu.VMEM((own_k, inner), F32),
            pltpu.VMEM((PLANES * rows, inner), BF16),
            pltpu.VMEM((PLANES * rows, inner), BF16),
            pltpu.VMEM((width, own_k), BF16),
            pltpu.VMEM((width, own_k), BF16),
            pltpu.VMEM((inner, inner), BF16),
            pltpu.VMEM((inner, inner), BF16),
            pltpu.VMEM((inner, inner), BF16),
            pltpu.VMEM((inner, inner), BF16),
            pltpu.VMEM((own_k, inner), BF16),
            pltpu.VMEM((own_k, inner), BF16),
            pltpu.VMEM((4, parts, rows // parts, inner), F32),
            pltpu.VMEM((8, inner), F32),
            pltpu.VMEM((4, 8, 128), F32),
            pltpu.VMEM((4, 8, 128), F32),
            pltpu.VMEM((4, 8, 128), F32),
            dma((4,)),
            dma((3,)),
            dma((3,)),
            dma(()),
            dma(()),
            dma((3,)),
            dma((3,)),
            dma(()),
            dma((CHUNKS,)),
            dma(()),
            dma((CHUNKS,)),
            dma((2, 2)),
            dma((2, HOPS)),
            dma((3, parts)),
            dma((2, parts)),
            dma((parts,)),
            dma((9,)),
            dma((9,)),
        ],
        compiler_params=pltpu.CompilerParams(
            collective_id=0, has_side_effects=True, vmem_limit_bytes=66_000_000
        ),
        name="precondition",
    )(
        grads[0, 0],
        jnp.transpose(basis_out, (0, 2, 1)),
        jnp.transpose(basis_in, (1, 0, 2)),
        eigvals,
        counts,
        slot_query[0],
    )
    live = (counts[0] > 0).astype(F32)
    return ((out[0] + out[1]) * live)[None, None], scores[0]


def solution(mesh):
    in_specs = (
        P(("layer", "expert"), None, "matrix", None),
        P("layer", None, ("expert", "matrix")),
        P("layer", ("expert", "matrix"), None),
        P("layer", ("expert", "matrix"), None),
        P(("layer", "expert")),
        P(("layer", "expert"), None),
    )
    out_specs = (P(("layer", "expert"), None, "matrix", None), P("layer"))
    return jax.shard_map(shards, mesh=mesh, in_specs=in_specs, out_specs=out_specs, check_vma=False)
```
